8 devices in a mesh: dp: 1 (over z), ep: 8 (over y, x, core).
Axes of the slice: x: 2, y: 2, z: 1, core: 2. Of those that a mesh axis runs over, the one named last changes fastest.
Arguments:
- tokens: bfloat16 [16384, 768], P(('dp', 'ep'))
- expert_idx: int32 [16384], P(('dp', 'ep'))
- w_router: float32 [768, 8], replicated
- w_in: bfloat16 [8, 768, 3072], P('ep')
- w_out: bfloat16 [8, 3072, 768], P('ep')
Outputs:
- output: bfloat16 [16384, 768], P(('dp', 'ep'))
All inputs are finite; a program needn't handle non-finite values.
Results may differ from the reference program's by a relative error of at most 0.001.
Values are sent between devices in bfloat16 or wider.
A program may use at most 1 GiB of HBM per device.

```python
import jax
import jax.numpy as jnp
from jax import lax

MODEL_DIM = 768
HIDDEN_DIM = 3072
NUM_EXPERTS = 8
GROUP_TOKENS = 2048
NUM_GROUPS = 8
CAPACITY = (5 * GROUP_TOKENS + 4 * NUM_EXPERTS - 1) // (4 * NUM_EXPERTS)
TOTAL_TOKENS = NUM_GROUPS * GROUP_TOKENS


def draw_choices(key):
    key_perm, key_shift, key_redraw, key_pick, key_hot = jax.random.split(key, 5)
    balanced = jnp.arange(GROUP_TOKENS, dtype=jnp.int32) % NUM_EXPERTS
    perm_keys = jax.random.split(key_perm, NUM_GROUPS)
    shuffled = jax.vmap(lambda perm_key: jax.random.permutation(perm_key, balanced))(perm_keys)
    group_shift = jax.random.randint(key_shift, (NUM_GROUPS, 1), 0, NUM_EXPERTS)
    choice = (shuffled + group_shift) % NUM_EXPERTS
    redraw = jax.random.randint(key_redraw, (NUM_GROUPS, GROUP_TOKENS), 0, 8) == 0
    picked = jax.random.randint(key_pick, (NUM_GROUPS, GROUP_TOKENS), 0, NUM_EXPERTS)
    choice = jnp.where(redraw, picked, choice)
    hot_expert = jax.random.randint(key_hot, (NUM_GROUPS, 1), 0, NUM_EXPERTS)
    leading = jnp.arange(GROUP_TOKENS)[None, :] <= CAPACITY
    choice = jnp.where(leading, hot_expert, choice)
    return choice.reshape(TOTAL_TOKENS).astype(jnp.int32)


def expert_weights(key, fan_in, fan_out, weight_scale):
    expert_keys = jax.random.split(key, NUM_EXPERTS)
    return lax.map(lambda one_key: (jax.random.normal(one_key, (fan_in, fan_out), jnp.float32) * weight_scale).astype(jnp.bfloat16), expert_keys)


def setup_inputs(seed: int = 0, part: int = 0) -> dict:
    root_key = jax.random.key(seed)
    key_tokens, key_choice, key_router, key_in, key_out = jax.random.split(root_key, 5)
    tokens = jax.random.normal(jax.random.fold_in(key_tokens, part), (TOTAL_TOKENS, MODEL_DIM), jnp.float32).astype(jnp.bfloat16)
    expert_idx = draw_choices(jax.random.fold_in(key_choice, part))
    w_router = jax.random.normal(key_router, (MODEL_DIM, NUM_EXPERTS), jnp.float32) * MODEL_DIM ** -0.5
    w_in = expert_weights(key_in, MODEL_DIM, HIDDEN_DIM, MODEL_DIM ** -0.5)
    w_out = expert_weights(key_out, HIDDEN_DIM, MODEL_DIM, NUM_EXPERTS * HIDDEN_DIM ** -0.5)
    return {"tokens": tokens, "expert_idx": expert_idx, "w_router": w_router, "w_in": w_in, "w_out": w_out}


def route_group(tok_rows, choice, w_router):
    logits = jnp.dot(tok_rows.astype(jnp.float32), w_router, precision=lax.Precision.HIGHEST)
    router_prob = jax.nn.softmax(logits, axis=-1)
    chosen = choice[:, None] == jnp.arange(NUM_EXPERTS, dtype=jnp.int32)[None, :]
    gate_prob = jnp.sum(jnp.where(chosen, router_prob, 0.0), axis=-1)
    running_count = jnp.cumsum(chosen.astype(jnp.int32), axis=0) - 1
    position = jnp.sum(jnp.where(chosen, running_count, 0), axis=-1)
    slot_index = jnp.where(position < CAPACITY, choice * CAPACITY + position, NUM_EXPERTS * CAPACITY)
    holder = jnp.full((NUM_EXPERTS * CAPACITY + 1,), GROUP_TOKENS, jnp.int32).at[slot_index].set(jnp.arange(GROUP_TOKENS, dtype=jnp.int32))
    buffer = jnp.take(tok_rows, holder[:-1], axis=0, mode="fill", fill_value=0)
    return buffer.reshape(NUM_EXPERTS, CAPACITY, MODEL_DIM), slot_index, gate_prob


def expert_apply(operands):
    rows_in, weight_in, weight_out = operands
    hidden = jnp.dot(rows_in, weight_in, preferred_element_type=jnp.float32)
    hidden_act = jax.nn.relu(hidden).astype(jnp.bfloat16)
    return jnp.dot(hidden_act, weight_out, preferred_element_type=jnp.float32).astype(jnp.bfloat16)


def combine_group(operands):
    flat_out, slot_rows, gate_rows = operands
    picked = jnp.take(flat_out, slot_rows, axis=0, mode="fill", fill_value=0)
    return (gate_rows[:, None] * picked.astype(jnp.float32)).astype(jnp.bfloat16)


def reference(tokens, expert_idx, w_router, w_in, w_out):
    grouped = tokens.reshape(NUM_GROUPS, GROUP_TOKENS, MODEL_DIM)
    choices = expert_idx.reshape(NUM_GROUPS, GROUP_TOKENS)
    buffers, slot_index, gate_prob = lax.map(lambda pair: route_group(pair[0], pair[1], w_router), (grouped, choices))
    per_expert = jnp.swapaxes(buffers, 0, 1).reshape(NUM_EXPERTS, NUM_GROUPS * CAPACITY, MODEL_DIM)
    expert_rows = lax.map(expert_apply, (per_expert, w_in, w_out))
    by_group = jnp.swapaxes(expert_rows.reshape(NUM_EXPERTS, NUM_GROUPS, CAPACITY, MODEL_DIM), 0, 1).reshape(NUM_GROUPS, NUM_EXPERTS * CAPACITY, MODEL_DIM)
    outputs = lax.map(combine_group, (by_group, slot_index, gate_prob))
    return outputs.reshape(TOTAL_TOKENS, MODEL_DIM)
```

```python
import functools

import jax
import jax.numpy as jnp
from jax import lax
from jax.experimental import pallas as pl
from jax.experimental.pallas import tpu as pltpu
from jax.sharding import PartitionSpec as P

MESH = pl.DeviceIdType.MESH
LANES = 128
F32 = jnp.float32
BF16 = jnp.bfloat16

SEND_ORDER = (6, 7, 2, 4, 3, 5, 1, 0)
WORK_ORDER = (0, 1, 6, 7, 2, 4, 3, 5)


def packed(order):
    return sum(k * 8**i for i, k in enumerate(order))


def partner(me, k):
    core = lax.rem(lax.rem(me, 2) + lax.rem(k, 2), 2)
    along_x = lax.rem(lax.rem(me // 2, 2) + lax.rem(k // 2, 2), 2)
    along_y = lax.rem(me // 4 + k // 4, 2)
    return along_y * 4 + along_x * 2 + core


def kernel(capacity, num_experts, x_hbm, idx_hbm, wr_hbm, w_in_hbm, w_out_hbm, y_hbm,
           x, idx, wr, w_in, w_out, onehot, hidden, code_rows, gate_rows, code_cols, gate_cols, acc,
           sent, recv, back, home, load_sem, store_sem, send_sem, recv_sem, back_sem, home_sem):
    me = lax.axis_index("ep")
    tokens, model_dim = x.shape
    hidden_dim = w_in.shape[1]
    tiles = tokens // LANES

    loads = [pltpu.make_async_copy(src, dst, load_sem.at[i]) for i, (src, dst) in enumerate(
        ((idx_hbm, idx), (x_hbm, x), (wr_hbm, wr), (w_in_hbm, w_in), (w_out_hbm, w_out)))]
    for load in loads:
        load.start()
    barrier = pltpu.get_barrier_semaphore()
    for k in range(1, num_experts):
        pl.semaphore_signal(barrier, inc=1, device_id={"ep": partner(me, k)}, device_id_type=MESH)

    def outward(k):
        return pltpu.make_async_remote_copy(sent.at[k], recv.at[k], send_sem.at[k], recv_sem.at[k], device_id={"ep": partner(me, k)}, device_id_type=MESH)

    def homeward(k):
        return pltpu.make_async_remote_copy(back.at[k], home.at[k], back_sem.at[k], home_sem.at[k], device_id={"ep": partner(me, k)}, device_id_type=MESH)

    loads[0].wait()
    choice = idx[...]
    rows = num_experts * tiles
    chosen = jnp.concatenate([(choice == e).astype(F32) for e in range(num_experts)], axis=0)
    row = lax.broadcasted_iota(jnp.int32, (rows, rows), 0)
    col = lax.broadcasted_iota(jnp.int32, (rows, rows), 1)
    earlier_tile = ((row // tiles == col // tiles) & (col < row)).astype(BF16)
    lane_row = lax.broadcasted_iota(jnp.int32, (LANES, LANES), 0)
    lane_col = lax.broadcasted_iota(jnp.int32, (LANES, LANES), 1)
    up_to = (lane_row <= lane_col).astype(BF16)
    chosen16 = chosen.astype(BF16)
    inside = jnp.dot(chosen16, up_to, preferred_element_type=F32)
    before = jnp.dot(earlier_tile, chosen16, preferred_element_type=F32)
    before = jnp.dot(before.astype(BF16), jnp.ones((LANES, LANES), BF16), preferred_element_type=F32)
    count = chosen * (inside + before)
    position = count[:tiles]
    for e in range(1, num_experts):
        position = position + count[e * tiles:(e + 1) * tiles]
    position = position.astype(jnp.int32) - 1
    code = jnp.where(position < capacity, choice * capacity + position, -(2**20))
    code_rows[...] = code

    loads[1].wait()

    def dispatch(step, order):
        k = lax.rem(order, 8)
        first = partner(me, k) * capacity
        slot = lax.broadcasted_iota(jnp.int32, (capacity, LANES), 0) + first
        for i in range(tiles):
            onehot[:, i * LANES:(i + 1) * LANES] = (slot == code_rows[i:i + 1, :]).astype(F32).astype(BF16)
        picked = jnp.dot(onehot[...], x[...], preferred_element_type=F32).astype(BF16)

        @pl.when(step < num_experts - 1)
        def _():
            sent[k] = picked

            @pl.when(step == 0)
            def _():
                pl.semaphore_wait(barrier, num_experts - 1)
            outward(k).start()

        @pl.when(step == num_experts - 1)
        def _():
            recv[0] = picked
        return order // 8

    lax.fori_loop(0, num_experts, dispatch, packed(SEND_ORDER))

    loads[2].wait()
    weight = wr[...]
    high = weight.astype(BF16)
    rest = weight - high.astype(F32)
    mid = rest.astype(BF16)
    low = (rest - mid.astype(F32)).astype(BF16)
    parts = [lax.dot_general(part, x[...], (((1,), (1,)), ((), ())), preferred_element_type=F32) for part in (low, mid, high)]
    logits = parts[0] + parts[1] + parts[2]
    top = jnp.max(logits, axis=0, keepdims=True)
    grown = jnp.exp(logits - top)
    total = jnp.sum(grown, axis=0, keepdims=True)
    prob = grown / total
    expert = lax.broadcasted_iota(jnp.int32, (num_experts, LANES), 0)
    for i in range(tiles):
        mine = expert == idx[i:i + 1, :]
        gate_rows[i:i + 1, :] = jnp.sum(jnp.where(mine, prob[:, i * LANES:(i + 1) * LANES], 0.0), axis=0, keepdims=True)
    pad = jnp.zeros((LANES - tiles, LANES), F32)
    code_t = jnp.concatenate([code_rows[...].astype(F32), pad], axis=0).T
    gate_t = jnp.concatenate([gate_rows[...], pad], axis=0).T
    for i in range(tiles):
        code_cols[i * LANES:(i + 1) * LANES, :] = jnp.broadcast_to(code_t[:, i:i + 1], (LANES, LANES)).astype(jnp.int32)
        gate_cols[i * LANES:(i + 1) * LANES, :] = jnp.broadcast_to(gate_t[:, i:i + 1], (LANES, LANES))

    loads[3].wait()
    loads[4].wait()
    chunk = hidden_dim // 3

    def expert_step(step, order):
        k = lax.rem(order, 8)

        @pl.when(step > 0)
        def _():
            outward(k).wait_recv()

        def up(n, carry):
            cols = pl.ds(pl.multiple_of(n * chunk, chunk), chunk)
            part = jnp.dot(recv[k], w_in[:, cols], preferred_element_type=F32)
            hidden[:, cols] = jnp.maximum(part, 0.0).astype(BF16)
            return carry

        lax.fori_loop(0, 3, up, 0)
        result = jnp.dot(hidden[...], w_out[...], preferred_element_type=F32).astype(BF16)

        @pl.when(step > 0)
        def _():
            back[k] = result
            homeward(k).start()

        @pl.when(step == 0)
        def _():
            home[0] = result
        return order // 8

    lax.fori_loop(0, num_experts, expert_step, packed(WORK_ORDER))

    tile = 256
    lane = lax.broadcasted_iota(jnp.int32, (tile, LANES), 1)
    lane_blocks = -(-capacity // LANES)

    def gathered(k, at):
        offset = code_cols[at, :] - partner(me, k) * capacity
        pick = jnp.concatenate([(offset == lane + b * LANES).astype(F32).astype(BF16) for b in range(lane_blocks)], axis=1)
        return jnp.dot(pick[:, :capacity], home[k], preferred_element_type=F32)

    def at_tile(t):
        return pl.ds(pl.multiple_of(t * tile, tile), tile)

    def combine(step, order):
        k = lax.rem(order, 8)

        @pl.when(step > 0)
        def _():
            homeward(k).wait_recv()

        def on_tile(t, carry):
            acc[at_tile(t), :] = (acc[at_tile(t), :].astype(F32) + gathered(k, at_tile(t))).astype(BF16)
            return carry

        lax.fori_loop(0, tokens // tile, on_tile, 0)
        return order // 8

    acc[...] = jnp.zeros_like(acc)
    lax.fori_loop(0, num_experts - 1, combine, packed(WORK_ORDER))
    last = WORK_ORDER[-1]
    homeward(last).wait_recv()

    def store(t):
        return pltpu.make_async_copy(acc.at[at_tile(t), :], y_hbm.at[at_tile(t), :], store_sem.at[t])

    def finish(t, carry):
        value = acc[at_tile(t), :].astype(F32) + gathered(last, at_tile(t))
        for b in range(model_dim // LANES):
            lanes = slice(b * LANES, (b + 1) * LANES)
            acc[at_tile(t), lanes] = (gate_cols[at_tile(t), :] * value[:, lanes]).astype(BF16)
        store(t).start()
        return carry

    lax.fori_loop(0, tokens // tile, finish, 0)
    for k in range(1, num_experts):
        outward(k).wait_send()
        homeward(k).wait_send()
    for t in range(tokens // tile):
        store(t).wait()


def solution(mesh):
    def local_block(tokens, expert_idx, w_router, w_in, w_out):
        tok_count, model_dim = tokens.shape
        local_experts, _, hidden_dim = w_in.shape
        num_experts = w_router.shape[1]
        capacity = (5 * tok_count + 4 * num_experts - 1) // (4 * num_experts)
        tiles = tok_count // LANES
        blocks = (num_experts, capacity, model_dim)
        anywhere = pl.BlockSpec(memory_space=pl.ANY)
        return pl.pallas_call(
            functools.partial(kernel, capacity, num_experts),
            out_shape=jax.ShapeDtypeStruct((tok_count, model_dim), BF16),
            in_specs=[anywhere] * 5,
            out_specs=anywhere,
            scratch_shapes=[
                pltpu.VMEM((tok_count, model_dim), BF16),
                pltpu.VMEM((tiles, LANES), jnp.int32),
                pltpu.VMEM((num_experts, model_dim), F32),
                pltpu.VMEM((model_dim, hidden_dim), BF16),
                pltpu.VMEM((hidden_dim, model_dim), BF16),
                pltpu.VMEM((capacity, tok_count), BF16),
                pltpu.VMEM((capacity, hidden_dim), BF16),
                pltpu.VMEM((tiles, LANES), jnp.int32),
                pltpu.VMEM((tiles, LANES), F32),
                pltpu.VMEM((tok_count, LANES), jnp.int32),
                pltpu.VMEM((tok_count, LANES), F32),
                pltpu.VMEM((tok_count, model_dim), BF16),
                pltpu.VMEM(blocks, BF16),
                pltpu.VMEM(blocks, BF16),
                pltpu.VMEM(blocks, BF16),
                pltpu.VMEM(blocks, BF16),
                pltpu.SemaphoreType.DMA((5,)),
                pltpu.SemaphoreType.DMA((tok_count // 256,)),
                pltpu.SemaphoreType.DMA((num_experts,)),
                pltpu.SemaphoreType.DMA((num_experts,)),
                pltpu.SemaphoreType.DMA((num_experts,)),
                pltpu.SemaphoreType.DMA((num_experts,)),
            ],
            compiler_params=pltpu.CompilerParams(collective_id=0, has_side_effects=True, vmem_limit_bytes=62 * 2**20),
            name="moe",
        )(tokens, expert_idx.reshape(tiles, LANES), w_router.T, w_in.reshape(model_dim, hidden_dim), w_out.reshape(hidden_dim, model_dim))

    return jax.shard_map(local_block, mesh=mesh, in_specs=(P(("dp", "ep"), None), P(("dp", "ep")), P(None, None), P("ep", None, None), P("ep", None, None)), out_specs=P(("dp", "ep"), None), check_vma=False)
```

```python
import functools

import jax
import jax.numpy as jnp
from jax import lax
from jax.experimental import pallas as pl
from jax.experimental.pallas import tpu as pltpu
from jax.sharding import PartitionSpec as P

MESH = pl.DeviceIdType.MESH
LANES = 128
F32 = jnp.float32
BF16 = jnp.bfloat16

PARTNERS = (0, 1, 6, 7, 2, 4, 3, 5)
REMOTE_FIRST = (2, 3, 4, 5, 6, 7, 1, 0)


def packed(order):
    return sum(k * 8**i for i, k in enumerate(order))


def partner(me, k):
    core = lax.rem(lax.rem(me, 2) + lax.rem(k, 2), 2)
    along_x = lax.rem(lax.rem(me // 2, 2) + lax.rem(k // 2, 2), 2)
    along_y = lax.rem(me // 4 + k // 4, 2)
    return along_y * 4 + along_x * 2 + core


def kernel(capacity, num_experts, x_hbm, idx_hbm, wr_hbm, w_in_hbm, w_out_hbm, y,
           x, idx, wr, w_in, w_out, onehot, hidden, code_rows, gate_rows, code_cols, gate_cols,
           sent, recv, back, home, tail, load_sem, send_sem, recv_sem, back_sem, home_sem):
    me = lax.axis_index("ep")
    tokens, model_dim = x.shape
    hidden_dim = w_in.shape[1]
    tiles = tokens // LANES
    half = capacity // 2
    main = home.shape[1]
    rest = tail.shape[1]

    load_idx, load_x, load_wr, load_in, load_out = [pltpu.make_async_copy(src, dst, load_sem.at[i]) for i, (src, dst) in enumerate(
        ((idx_hbm, idx), (x_hbm, x), (wr_hbm, wr), (w_in_hbm, w_in), (w_out_hbm, w_out)))]
    load_idx.start()
    load_x.start()
    load_wr.start()
    barrier = pltpu.get_barrier_semaphore()
    for k in range(1, num_experts):
        pl.semaphore_signal(barrier, inc=1, device_id={"ep": partner(me, k)}, device_id_type=MESH)

    def remote(src, dst, sem_a, sem_b, k):
        return pltpu.make_async_remote_copy(src, dst, sem_a, sem_b, device_id={"ep": partner(me, k)}, device_id_type=MESH)

    def outward(s, h, k):
        rows = pl.ds(pl.multiple_of(h * half, half), half)
        return remote(sent.at[s, rows], recv.at[s, rows], send_sem.at[s, h], recv_sem.at[s, h], k)

    def homeward(s, k):
        return remote(back.at[s, :main], home.at[s], back_sem.at[s, 0], home_sem.at[s, 0], k)

    def homeward_rest(s, k):
        return remote(back.at[s, main:], tail.at[s], back_sem.at[s, 1], home_sem.at[s, 1], k)

    load_idx.wait()
    choice = idx[...]
    chosen = jnp.concatenate([(choice == partner(me, k)).astype(F32) for k in PARTNERS], axis=0)
    rows = num_experts * tiles
    row = lax.broadcasted_iota(jnp.int32, (rows, rows), 0)
    col = lax.broadcasted_iota(jnp.int32, (rows, rows), 1)
    earlier_tile = ((row // tiles == col // tiles) & (col < row)).astype(BF16)
    lane_row = lax.broadcasted_iota(jnp.int32, (LANES, LANES), 0)
    lane_col = lax.broadcasted_iota(jnp.int32, (LANES, LANES), 1)
    up_to = (lane_row <= lane_col).astype(BF16)
    chosen16 = chosen.astype(BF16)
    inside = jnp.dot(chosen16, up_to, preferred_element_type=F32)
    before = jnp.dot(earlier_tile, chosen16, preferred_element_type=F32)
    before = jnp.dot(before.astype(BF16), jnp.ones((LANES, LANES), BF16), preferred_element_type=F32)
    position = (inside + before).astype(jnp.int32) - 1
    code = jnp.full((tiles, LANES), -1, jnp.int32)
    for s in range(num_experts):
        at = slice(s * tiles, (s + 1) * tiles)
        code = jnp.where((chosen[at] > 0.0) & (position[at] < capacity), position[at] + s * capacity, code)
    code_rows[...] = code

    load_x.wait()
    load_in.start()
    load_out.start()

    def dispatch(step, carry):
        steps, order = carry
        s, k, h = lax.rem(steps, 8), lax.rem(order, 8), lax.rem(step, 2)
        slot = lax.broadcasted_iota(jnp.int32, (half, LANES), 0) + (s * capacity + h * half)
        for i in range(tiles):
            onehot[:, i * LANES:(i + 1) * LANES] = (slot == code_rows[i:i + 1, :]).astype(F32).astype(BF16)
        picked = jnp.dot(onehot[...], x[...], preferred_element_type=F32).astype(BF16)
        there = pl.ds(pl.multiple_of(h * half, half), half)

        @pl.when(step < 2 * num_experts - 2)
        def _():
            sent[s, there] = picked

            @pl.when(step == 0)
            def _():
                pl.semaphore_wait(barrier, num_experts - 1)
            outward(s, h, k).start()

        @pl.when(step >= 2 * num_experts - 2)
        def _():
            recv[0, there] = picked
        return jnp.where(h == 1, steps // 8, steps), jnp.where(h == 1, order // 8, order)

    lax.fori_loop(0, 2 * num_experts, dispatch, (packed(REMOTE_FIRST), packed([PARTNERS[s] for s in REMOTE_FIRST])))

    load_wr.wait()
    weight = wr[...]
    high = weight.astype(BF16)
    left = weight - high.astype(F32)
    mid = left.astype(BF16)
    low = (left - mid.astype(F32)).astype(BF16)
    parts = [lax.dot_general(part, x[...], (((1,), (1,)), ((), ())), preferred_element_type=F32) for part in (low, mid, high)]
    logits = parts[0] + parts[1] + parts[2]
    top = jnp.max(logits, axis=0, keepdims=True)
    grown = jnp.exp(logits - top)
    total = jnp.sum(grown, axis=0, keepdims=True)
    prob = grown / total
    expert = lax.broadcasted_iota(jnp.int32, (num_experts, LANES), 0)
    for i in range(tiles):
        mine = expert == idx[i:i + 1, :]
        gate_rows[i:i + 1, :] = jnp.sum(jnp.where(mine, prob[:, i * LANES:(i + 1) * LANES], 0.0), axis=0, keepdims=True)
    pad = jnp.zeros((LANES - tiles, LANES), F32)
    code_t = jnp.concatenate([code_rows[...].astype(F32), pad], axis=0).T
    gate_t = jnp.concatenate([gate_rows[...], pad], axis=0).T
    for i in range(tiles):
        code_cols[i * LANES:(i + 1) * LANES, :] = jnp.broadcast_to(code_t[:, i:i + 1], (LANES, LANES)).astype(jnp.int32)
        gate_cols[i * LANES:(i + 1) * LANES, :] = jnp.broadcast_to(gate_t[:, i:i + 1], (LANES, LANES))

    load_in.wait()
    load_out.wait()
    chunk = hidden_dim // 3

    def expert_step(s, order):
        k = lax.rem(order, 8)

        @pl.when(s > 0)
        def _():
            outward(s, 0, k).wait_recv()
            outward(s, 1, k).wait_recv()

        def up(n, carry):
            cols = pl.ds(pl.multiple_of(n * chunk, chunk), chunk)
            part = jnp.dot(recv[s], w_in[:, cols], preferred_element_type=F32)
            hidden[:, cols] = jnp.maximum(part, 0.0).astype(BF16)
            return carry

        lax.fori_loop(0, 3, up, 0)
        result = jnp.dot(hidden[...], w_out[...], preferred_element_type=F32).astype(BF16)

        @pl.when(s > 0)
        def _():
            back[s] = result
            homeward(s, k).start()
            homeward_rest(s, k).start()

        @pl.when(s == 0)
        def _():
            home[0] = result[:main]
            tail[0] = result[main:]
        return order // 8

    lax.fori_loop(0, num_experts, expert_step, packed(PARTNERS))

    tile = 512
    lane = lax.broadcasted_iota(jnp.int32, (1, LANES), 1)

    def gathered(at, targets, block):
        pick = jnp.concatenate([(code_cols[at, :] == target).astype(F32).astype(BF16) for target in targets], axis=1)
        return jnp.dot(pick, block, preferred_element_type=F32)

    def at_tile(t):
        return pl.ds(pl.multiple_of(t * tile, tile), tile)

    def add(targets, block):
        def on_tile(t, carry):
            y[at_tile(t), :] = y[at_tile(t), :] + gathered(at_tile(t), targets, block).astype(BF16)
            return carry
        lax.fori_loop(0, tokens // tile, on_tile, 0)

    def combine(s, order):
        k = lax.rem(order, 8)

        @pl.when(s > 0)
        def _():
            homeward(s, k).wait_recv()
        add([lane + (s * capacity + b * LANES) for b in range(main // LANES)], home[s])
        return order // 8

    def rest_targets(first):
        out = []
        for b in range(2):
            within = lane + b * LANES
            out.append((first + within // rest) * capacity + main + lax.rem(within, rest))
        return out

    y[...] = jnp.zeros_like(y)
    split = num_experts - 2
    lax.fori_loop(0, split, combine, packed(PARTNERS[:split]))
    count = 2 * LANES // rest
    for s in range(1, count):
        homeward_rest(s, PARTNERS[s]).wait_recv()
    add(rest_targets(0), tail[:count].reshape(2 * LANES, model_dim))
    lax.fori_loop(split, num_experts, combine, packed(PARTNERS[split:]))
    for s in range(count, num_experts):
        homeward_rest(s, PARTNERS[s]).wait_recv()

    def finish(t, carry):
        value = y[at_tile(t), :].astype(F32) + gathered(at_tile(t), rest_targets(count), tail[count:].reshape(2 * LANES, model_dim))
        for b in range(model_dim // LANES):
            lanes = slice(b * LANES, (b + 1) * LANES)
            y[at_tile(t), lanes] = (gate_cols[at_tile(t), :] * value[:, lanes]).astype(BF16)
        return carry

    lax.fori_loop(0, tokens // tile, finish, 0)
    for s in range(1, num_experts):
        outward(s, 0, PARTNERS[s]).wait_send()
        outward(s, 1, PARTNERS[s]).wait_send()
        homeward(s, PARTNERS[s]).wait_send()
        homeward_rest(s, PARTNERS[s]).wait_send()


def solution(mesh):
    def local_block(tokens, expert_idx, w_router, w_in, w_out):
        tok_count, model_dim = tokens.shape
        local_experts, _, hidden_dim = w_in.shape
        num_experts = w_router.shape[1]
        capacity = (5 * tok_count + 4 * num_experts - 1) // (4 * num_experts)
        tiles = tok_count // LANES
        main = 2 * LANES
        in_hbm = pl.BlockSpec(memory_space=pltpu.HBM)
        return pl.pallas_call(
            functools.partial(kernel, capacity, num_experts),
            out_shape=pltpu.VMEM((tok_count, model_dim), BF16),
            in_specs=[in_hbm] * 5,
            out_specs=pl.BlockSpec(memory_space=pltpu.VMEM),
            scratch_shapes=[
                pltpu.VMEM((tok_count, model_dim), BF16),
                pltpu.VMEM((tiles, LANES), jnp.int32),
                pltpu.VMEM((num_experts, model_dim), F32),
                pltpu.VMEM((model_dim, hidden_dim), BF16),
                pltpu.VMEM((hidden_dim, model_dim), BF16),
                pltpu.VMEM((capacity // 2, tok_count), BF16),
                pltpu.VMEM((capacity, hidden_dim), BF16),
                pltpu.VMEM((tiles, LANES), jnp.int32),
                pltpu.VMEM((tiles, LANES), F32),
                pltpu.VMEM((tok_count, LANES), jnp.int32),
                pltpu.VMEM((tok_count, LANES), F32),
                pltpu.VMEM((num_experts, capacity, model_dim), BF16),
                pltpu.VMEM((num_experts, capacity, model_dim), BF16),
                pltpu.VMEM((num_experts, capacity, model_dim), BF16),
                pltpu.VMEM((num_experts, main, model_dim), BF16),
                pltpu.VMEM((num_experts, capacity - main, model_dim), BF16),
                pltpu.SemaphoreType.DMA((5,)),
                pltpu.SemaphoreType.DMA((num_experts, 2)),
                pltpu.SemaphoreType.DMA((num_experts, 2)),
                pltpu.SemaphoreType.DMA((num_experts, 2)),
                pltpu.SemaphoreType.DMA((num_experts, 2)),
            ],
            compiler_params=pltpu.CompilerParams(collective_id=0, has_side_effects=True, vmem_limit_bytes=48 * 2**20),
            name="moe",
        )(*[pltpu.with_memory_space_constraint(a, pltpu.HBM) for a in (
            tokens, expert_idx.reshape(tiles, LANES), w_router.T, w_in.reshape(model_dim, hidden_dim), w_out.reshape(hidden_dim, model_dim))])

    return jax.shard_map(local_block, mesh=mesh, in_specs=(P(("dp", "ep"), None), P(("dp", "ep")), P(None, None), P("ep", None, None), P("ep", None, None)), out_specs=P(("dp", "ep"), None), check_vma=False)
```
